32 devices in a mesh: row: 8 (over y, x, core), gz: 4 (over z).
Axes of the slice: x: 2, y: 2, z: 4, core: 2. Of those that a mesh axis runs over, the one named last changes fastest.
Arguments:
- velocity_x: bfloat16 [2, 8, 1024, 1024], P(None, None, 'row', 'gz'), may hold values from -6 to 6
- velocity_y: bfloat16 [2, 8, 1024, 1024], P(None, None, 'row', 'gz'), may hold values from -6 to 6
- velocity_z: bfloat16 [2, 8, 1024, 1024], P(None, None, 'row', 'gz'), may hold values from -6 to 6
- spacing: float32 [64], replicated, may hold values from 0.5 to 2
- level_index: int32 [1024], replicated, may hold values from 0 to 63
- plane_index: int32 [8], replicated, may hold values from 4 to 128
Outputs:
- pressure: float32 [2, 8, 1024, 1024], P(None, None, 'row', 'gz')
The draws below stay inside these ranges and needn't reach their ends.
All inputs are finite; a program needn't handle non-finite values.
Results may differ from the reference program's by a relative error of at most 0.002.
The reference program's roundings to bfloat16 on the way count: a program that leaves them out, or rounds other values in their place, can miss the bound.
Values may be sent and summed in bfloat16 or wider, within the bound.
No kernel may reach another device: no remote copies, remote signals or barrier semaphores. Data moves between devices by JAX's collectives and lax.ppermute only.
A program may use at most 64 MiB of HBM per device.

```python
import math
import jax
import jax.numpy as jnp
from jax import lax

NX = 1024
NZ = 1024
NLEV = 64
P_SIZE = 8


def plant(values, rng, low, largest):
    dims = values.shape
    spot = [jax.random.randint(jax.random.fold_in(rng, axis), (), 0, dims[axis]) for axis in range(len(dims))]
    values = values.at[tuple(spot)].set(low)
    longest = dims.index(max(dims))
    spot[longest] = (spot[longest] + 1) % dims[longest]
    return values.at[tuple(spot)].set(largest)


def shard_levels(own_key, shape, cuts, low, high):
    factor_of, own = 1.0, jax.random.fold_in(own_key, 6)
    for position, shards_of in cuts:
        heights = jnp.exp(jax.random.uniform(jax.random.fold_in(own, position), (shards_of,), jnp.float32, low / len(cuts), high / len(cuts)))
        factor_of = factor_of * jnp.repeat(heights, shape[position] // shards_of).reshape([-1 if axis == position else 1 for axis in range(len(shape))])
    return factor_of


def centred(key, dims, deviation, limit, split=(), kind=jnp.bfloat16):
    level = shard_levels(key, dims, split, -0.22, 0.18) if split else 1.0
    array = jax.random.normal(key, dims, jnp.float32) * deviation * level
    return jnp.minimum(jnp.maximum(array, -limit), limit).astype(kind)


def setup_inputs(seed: int = 0) -> dict:
    key_of = jax.random.split(jax.random.key(seed), 7)
    velocity_x = centred(key_of[0], (2, P_SIZE, NX, NZ), 1.0, 6.0, ((2, 8), (3, 4)))
    velocity_y = centred(key_of[1], (2, P_SIZE, NX, NZ), 1.0, 6.0, ((2, 8), (3, 4)))
    velocity_z = centred(key_of[2], (2, P_SIZE, NX, NZ), 1.0, 6.0, ((2, 8), (3, 4)))
    spacing = jnp.clip(jnp.exp(jax.random.uniform(key_of[3], (NLEV,), jnp.float32, math.log(0.5), math.log(2.0))), 0.5, 2.0)
    level_index = plant(jax.random.randint(key_of[4], (NZ,), 0, NLEV), jax.random.fold_in(key_of[4], 1), 0, NLEV - 1).astype(jnp.int32)
    plane_index = plant(jax.random.randint(key_of[5], (P_SIZE,), 4, 129), jax.random.fold_in(key_of[5], 1), 4, 128).astype(jnp.int32)
    return {"velocity_x": velocity_x, "velocity_y": velocity_y, "velocity_z": velocity_z, "spacing": spacing, "level_index": level_index, "plane_index": plane_index}


full_turn = 2.0 * math.pi
wave_unit = 2.0 * math.pi / 2048.0


def band_coefficients(cell_width):
    length = cell_width.shape[0]
    index = jnp.arange(length, dtype=jnp.int32)
    previous = jnp.concatenate([cell_width[:1], cell_width[:-1]])
    following = jnp.concatenate([cell_width[1:], cell_width[-1:]])
    lower_band = jnp.where(index > 0, 1.0 / (0.5 * (previous + cell_width) * cell_width), 0.0)
    upper_band = jnp.where(index < length - 1, 1.0 / (0.5 * (cell_width + following) * cell_width), 0.0)
    return lower_band, upper_band


def thomas(lower_band, diagonal, upper_band, right_real, right_imag):
    rows = (lower_band, upper_band, diagonal.T, right_real.T, right_imag.T)

    def sweep(carry, row):
        ratio_prev, real_prev, imag_prev = carry
        low_coef, up_coef, diag_col, real_in, imag_in = row
        pivot = diag_col - low_coef * ratio_prev
        ratio = up_coef / pivot
        real_now = (real_in - low_coef * real_prev) / pivot
        imag_now = (imag_in - low_coef * imag_prev) / pivot
        return (ratio, real_now, imag_now), (ratio, real_now, imag_now)

    zeros = jnp.zeros((diagonal.shape[0],), diagonal.dtype)
    unused, (ratios, reals, imags) = lax.scan(sweep, (zeros, zeros, zeros), rows)

    def back(carry, row):
        next_real, next_imag = carry
        ratio, real_now, imag_now = row
        value_real = real_now - ratio * next_real
        value_imag = imag_now - ratio * next_imag
        return (value_real, value_imag), (value_real, value_imag)

    unused, (sol_real, sol_imag) = lax.scan(back, (zeros, zeros), (ratios, reals, imags), reverse=True)
    return sol_real.T, sol_imag.T


def reference(velocity_x, velocity_y, velocity_z, spacing, level_index, plane_index):
    cell_width = spacing[level_index]
    lower_band, upper_band = band_coefficients(cell_width)
    modes = jnp.arange(NX, dtype=jnp.int32)
    signed = jnp.where(modes >= NX // 2, modes - NX, modes)
    wave_x = signed.astype(jnp.float32) * (full_turn / NX)

    def one_plane(item):
        along, across, upward, index_y = item
        wave_y = index_y.astype(jnp.float32) * wave_unit
        up_real = upward[0].astype(jnp.float32)
        up_imag = upward[1].astype(jnp.float32)
        zero_col = jnp.zeros((NX, 1), jnp.float32)
        below_real = jnp.concatenate([zero_col, up_real[:, :-1]], axis=1)
        below_imag = jnp.concatenate([zero_col, up_imag[:, :-1]], axis=1)
        across_real = across[0].astype(jnp.float32)
        across_imag = across[1].astype(jnp.float32)
        source_real = (-wave_y * across_imag + (up_real - below_real) / cell_width).astype(jnp.bfloat16)
        source_imag = (wave_y * across_real + (up_imag - below_imag) / cell_width).astype(jnp.bfloat16)
        source_real, source_imag = lax.optimization_barrier((source_real, source_imag))
        source_hat = jnp.fft.fft(source_real.astype(jnp.float32) + 1j * source_imag.astype(jnp.float32), axis=0)
        along_hat = jnp.fft.fft(along[0].astype(jnp.float32) + 1j * along[1].astype(jnp.float32), axis=0)
        right_hat = source_hat + 1j * wave_x[:, None] * along_hat
        wave_sq = wave_x * wave_x + wave_y * wave_y
        diagonal = -(lower_band + upper_band)[None, :] - wave_sq[:, None]
        sol_real, sol_imag = thomas(lower_band, diagonal, upper_band, jnp.real(right_hat), jnp.imag(right_hat))
        field = jnp.fft.ifft(sol_real + 1j * sol_imag, axis=0)
        return jnp.stack([jnp.real(field), jnp.imag(field)]).astype(jnp.float32)

    stacked = lax.map(one_plane, (jnp.moveaxis(velocity_x, 1, 0), jnp.moveaxis(velocity_y, 1, 0), jnp.moveaxis(velocity_z, 1, 0), plane_index))
    return jnp.moveaxis(stacked, 0, 1)
```

```python
import functools
import math

import jax
import jax.numpy as jnp
from jax import lax
from jax.experimental import pallas as pl
from jax.experimental.pallas import tpu as pltpu
from jax.sharding import PartitionSpec as P


RADIX = 8
full_turn = 2.0 * math.pi
wave_unit = 2.0 * math.pi / 2048.0
f32 = jnp.float32
bf16 = jnp.bfloat16
VMEM = pl.BlockSpec(memory_space=pltpu.VMEM)
SMEM = pl.BlockSpec(memory_space=pltpu.SMEM)
ANY = pl.BlockSpec(memory_space=pl.ANY)
NT = (((1,), (1,)), ((), ()))
NN = (((1,), (0,)), ((), ()))


def shape_of(dims, dtype):
    return jax.ShapeDtypeStruct(dims, dtype)


def call(kernel, out_shape, in_specs, scratch=(), flops=1e8, mib=24, out_specs=None):
    if out_specs is None:
        out_specs = jax.tree.map(lambda _: VMEM, out_shape)
    return pl.pallas_call(
        kernel,
        out_shape=out_shape,
        in_specs=in_specs,
        out_specs=out_specs,
        scratch_shapes=list(scratch),
        compiler_params=pltpu.CompilerParams(vmem_limit_bytes=mib << 20),
        cost_estimate=pl.CostEstimate(
            flops=int(flops), bytes_accessed=1 << 20, transcendentals=0
        ),
    )


def rows8(index):
    return pl.ds(pl.multiple_of(index * 8, 8), 8)


def butterfly(re, im, sign):
    half = math.sqrt(0.5)
    sr = [re[j] + re[j + 4] for j in range(4)]
    si = [im[j] + im[j + 4] for j in range(4)]
    dr = [re[j] - re[j + 4] for j in range(4)]
    di = [im[j] - im[j + 4] for j in range(4)]

    def turn(a, b):
        return (-b, a) if sign > 0 else (b, -a)

    def four(ar, ai):
        c0r, c0i = ar[0] + ar[2], ai[0] + ai[2]
        c1r, c1i = ar[0] - ar[2], ai[0] - ai[2]
        d0r, d0i = ar[1] + ar[3], ai[1] + ai[3]
        d1r, d1i = turn(ar[1] - ar[3], ai[1] - ai[3])
        return (
            [c0r + d0r, c1r + d1r, c0r - d0r, c1r - d1r],
            [c0i + d0i, c1i + d1i, c0i - d0i, c1i - d1i],
        )

    t1r, t1i = turn(dr[1], di[1])
    t3r, t3i = turn(dr[3], di[3])
    br = [dr[0], (dr[1] + t1r) * half, None, (t3r - dr[3]) * half]
    bi = [di[0], (di[1] + t1i) * half, None, (t3i - di[3]) * half]
    br[2], bi[2] = turn(dr[2], di[2])
    even_r, even_i = four(sr, si)
    odd_r, odd_i = four(br, bi)
    out_r = [None] * 8
    out_i = [None] * 8
    for q in range(4):
        out_r[2 * q], out_i[2 * q] = even_r[q], even_i[q]
        out_r[2 * q + 1], out_i[2 * q + 1] = odd_r[q], odd_i[q]
    return out_r, out_i


def split(values):
    high = values.astype(bf16)
    low = (values - high.astype(f32)).astype(bf16)
    return high, low


def pack_kernel(rows, me, u_ref, w_ref, wall_ref, *pieces):
    parts, planes, xb, _ = u_ref.shape
    for s in range(rows):
        pieces[s][...] = u_ref[:, me[0] ^ s]
    lane = lax.broadcasted_iota(jnp.int32, (parts * planes, 128), 1)
    line = lax.broadcasted_iota(jnp.int32, (parts * planes, 128), 0)
    total = jnp.zeros((parts * planes, xb), f32)
    for c in range(parts):
        for p in range(planes):
            pick = ((lane == 127) & (line == c * planes + p)).astype(f32).astype(bf16)
            total = total + lax.dot_general(
                pick, w_ref[c, p], NT, preferred_element_type=f32
            )
    wall_ref[...] = total.astype(bf16)


def source_kernel(rows, me, wave_y, v_ref, w_ref, wall_ref, width_ref, *rest):
    pieces, held = rest[:rows], rest[rows]
    parts, planes, xb, depth = v_ref.shape
    wall = jnp.transpose(wall_ref[...].astype(f32))
    lane = lax.broadcasted_iota(jnp.int32, (xb, depth), 1)
    width = jnp.broadcast_to(width_ref[...], (xb, depth))
    for p in range(planes):
        for c in range(parts):
            w = w_ref[c, p].astype(f32)
            column = wall[:, c * planes + p : c * planes + p + 1]
            below = jnp.where(lane == 0, column, pltpu.roll(w, 1, 1))
            slope = (w - below) / width
            across = wave_y[p] * v_ref[1 - c, p].astype(f32)
            total = slope - across if c == 0 else across + slope
            held[p, c] = total.astype(bf16)
    for s in range(rows):
        pieces[s][...] = held[me[0] ^ s]


def prepare_kernel(
    total_x, lower, upper, wave_ref, gate, thi, tlo, inv, alp, cut, mid, aa, bb
):
    inner = total_x // RADIX
    depth = lower.shape[0]
    middle = depth // 2
    norm = 1.0 / math.sqrt(total_x)
    row = lax.broadcasted_iota(jnp.int32, (inner, inner), 0)
    col = lax.broadcasted_iota(jnp.int32, (inner, inner), 1)
    for k1 in range(RADIX):
        turn = (row * (RADIX * col + k1)) % total_x
        turn = jnp.where(turn >= total_x // 2, turn - total_x, turn)
        angle = turn.astype(f32) * (full_turn / total_x)
        ch, cl = split(jnp.cos(angle) * norm)
        sh, sl = split(jnp.sin(angle) * norm)
        for table, cosine, sine in ((thi, ch, sh), (tlo, cl, sl)):
            table[k1, :inner, :inner] = cosine
            table[k1, :inner, inner:] = -sine
            table[k1, inner:, :inner] = sine
            table[k1, inner:, inner:] = cosine

    wave_sq = wave_ref[...]
    zero = jnp.zeros((RADIX, inner), f32)

    def factor(i, carry):
        c_low, c_up, a_prev, b_prev = carry
        j, t = i, depth - 1 - i
        d_j = -(lower[j] + upper[j]) - wave_sq
        d_t = -(lower[t] + upper[t]) - wave_sq
        inv_j = 1.0 / (d_j - lower[j] * c_low)
        inv_t = 1.0 / (d_t - upper[t] * c_up)
        alp_j, alp_t = lower[j] * inv_j, upper[t] * inv_t
        c_low, c_up = upper[j] * inv_j, lower[t] * inv_t
        inv[rows8(j), :] = inv_j
        inv[rows8(t), :] = inv_t
        alp[rows8(j), :] = alp_j
        alp[rows8(t), :] = alp_t
        cut[rows8(j), :] = c_low
        cut[rows8(t), :] = c_up
        a_prev = -alp_j * a_prev
        b_prev = -alp_t * b_prev
        aa[rows8(j), :] = a_prev
        bb[rows8(t), :] = b_prev
        return c_low, c_up, a_prev, b_prev

    one = zero + 1.0
    c_low, c_up, a_mid, b_mid = lax.fori_loop(
        0, middle, factor, (zero, zero, one, one), unroll=4
    )
    join = 1.0 / (1.0 - c_low * c_up)
    mid[...] = join
    a_low = a_mid * join
    a_up = -c_up * a_low
    b_low = -c_low * b_mid * join
    b_up = b_mid - c_up * b_low
    j, t = middle - 1, middle
    aa[rows8(j), :] = a_low
    aa[rows8(t), :] = a_up
    bb[rows8(j), :] = b_low
    bb[rows8(t), :] = b_up

    def outward(i, carry):
        a_low, a_up, b_low, b_up = carry
        j, t = middle - 1 - i, middle + i
        c_j, c_t = cut[rows8(j), :], cut[rows8(t), :]
        a_low = aa[rows8(j), :] - c_j * a_low
        b_low = -c_j * b_low
        a_up = -c_t * a_up
        b_up = bb[rows8(t), :] - c_t * b_up
        aa[rows8(j), :] = a_low
        aa[rows8(t), :] = a_up
        bb[rows8(j), :] = b_low
        bb[rows8(t), :] = b_up
        return a_low, a_up, b_low, b_up

    lax.fori_loop(1, middle, outward, (a_low, a_up, b_low, b_up), unroll=4)


def short_transform(rows, me, pieces, thi, tlo, held, turned, yhi, ylo, store):
    radix, parts, inner, depth = held.shape
    xb = pieces[0].shape[1]
    for s in range(rows):
        start = (me[0] ^ s) * xb
        group = start // inner
        offset = pl.multiple_of(start % inner, xb)
        held[group, :, pl.ds(offset, xb), :] = pieces[s][...]
    line = lax.broadcasted_iota(jnp.int32, (depth, depth), 0)
    lane = lax.broadcasted_iota(jnp.int32, (depth, depth), 1)
    unit = (line == lane).astype(f32).astype(bf16)
    for r in range(radix):
        block = held[r].reshape(parts * inner, depth)
        turned[r] = lax.dot_general(unit, block, NT, preferred_element_type=f32)

    def mix(i, carry):
        at = pl.ds(pl.multiple_of(i * 16, 16), 16)
        re = [turned[r, at, :inner] for r in range(radix)]
        im = [turned[r, at, inner:] for r in range(radix)]
        re, im = butterfly(re, im, -1)
        for k1 in range(radix):
            high, low = split(re[k1])
            yhi[k1, at, :inner] = high
            ylo[k1, at, :inner] = low
            high, low = split(im[k1])
            yhi[k1, at, inner:] = high
            ylo[k1, at, inner:] = low
        return carry

    lax.fori_loop(0, depth // 16, mix, 0)
    for k1 in range(radix):
        dot = functools.partial(
            lax.dot_general, dimension_numbers=NN, preferred_element_type=f32
        )
        out = (
            dot(yhi[k1], thi[k1]) + dot(ylo[k1], thi[k1]) + dot(yhi[k1], tlo[k1])
        )
        store(k1, out)


def along_kernel(rows, me, wave_ref, thi, tlo, *rest):
    pieces = rest[:rows]
    gre, gim, held, turned, yhi, ylo = rest[rows:]
    depth, inner = held.shape[3], held.shape[2]

    def store(k1, out):
        wave = wave_ref[k1 : k1 + 1, :]
        re = out[:, inner:] * -wave
        im = out[:, :inner] * wave
        for z in range(0, depth, 8):
            gre[pl.ds(8 * z + k1, 8, stride=8), :] = re[z : z + 8]
            gim[pl.ds(8 * z + k1, 8, stride=8), :] = im[z : z + 8]

    short_transform(rows, me, pieces, thi, tlo, held, turned, yhi, ylo, store)


def solve_kernel(rows, me, thi, tlo, inv, alp, cut, mid, aa, bb, gre, gim, *rest):
    pieces = rest[:rows]
    yre, yim, edges, held, turned, yhi, ylo, sre, sim = rest[rows:]
    depth, inner = held.shape[3], held.shape[2]
    middle = depth // 2

    def store(k1, out):
        for z in range(0, depth, 8):
            sre[pl.ds(8 * z + k1, 8, stride=8), :] = out[z : z + 8, :inner]
            sim[pl.ds(8 * z + k1, 8, stride=8), :] = out[z : z + 8, inner:]

    short_transform(rows, me, pieces, thi, tlo, held, turned, yhi, ylo, store)

    def inward(i, carry):
        out = []
        for side, row in enumerate((i, depth - 1 - i)):
            at = rows8(row)
            scale, back = inv[at, :], alp[at, :]
            re = (sre[at, :] + gre[at, :]) * scale - back * carry[2 * side]
            im = (sim[at, :] + gim[at, :]) * scale - back * carry[2 * side + 1]
            sre[at, :] = re
            sim[at, :] = im
            out += [re, im]
        return tuple(out)

    zero = jnp.zeros((8, inner), f32)
    low_re, low_im, up_re, up_im = lax.fori_loop(
        0, middle, inward, (zero,) * 4, unroll=4
    )
    j, t = rows8(middle - 1), rows8(middle)
    c_j, c_t, join = cut[j, :], cut[t, :], mid[...]
    low_re = (low_re - c_j * up_re) * join
    low_im = (low_im - c_j * up_im) * join
    up_re = up_re - c_t * low_re
    up_im = up_im - c_t * low_im
    yre[j, :] = low_re
    yim[j, :] = low_im
    yre[t, :] = up_re
    yim[t, :] = up_im

    def outward(i, carry):
        out = []
        for side, row in enumerate((middle - 1 - i, middle + i)):
            at = rows8(row)
            back = cut[at, :]
            re = sre[at, :] - back * carry[2 * side]
            im = sim[at, :] - back * carry[2 * side + 1]
            yre[at, :] = re
            yim[at, :] = im
            out += [re, im]
        return tuple(out)

    low_re, low_im, up_re, up_im = lax.fori_loop(
        1, middle, outward, (low_re, low_im, up_re, up_im), unroll=4
    )
    top = rows8(depth - 1)
    values = (aa[:8], aa[top, :], bb[:8], bb[top, :], low_re, up_re, low_im, up_im)
    for slot, value in enumerate(values):
        edges[8 * slot : 8 * slot + 8, :] = value


def back_kernel(rows, groups, me, thi, tlo, aa, bb, yre, yim, *rest):
    edges = rest[:groups]
    pieces = rest[groups : groups + rows]
    table, firsts, lasts, pre, pim, phi, plo, mixed, done = rest[groups + rows :]
    radix, parts, inner, depth = done.shape
    xb = pieces[0].shape[1]
    own = me[1]
    for s in range(groups):
        table[own ^ s] = edges[s][...]

    zero = jnp.zeros((8, inner), f32)
    eliminated = []
    last_re, last_im, last_by = zero, zero, zero
    for g in range(groups):
        af, at, bf, bt, fr, tr, fi, ti = (
            table[g, 8 * slot : 8 * slot + 8, :] for slot in range(8)
        )
        scale = 1.0 / (1.0 - af * last_by)
        first_re = (fr + af * last_re) * scale
        first_im = (fi + af * last_im) * scale
        first_by = bf * scale
        through = at * last_by
        eliminated.append((first_re, first_im, first_by, last_re, last_im, last_by))
        last_re, last_im, last_by = (
            tr + at * last_re + through * first_re,
            ti + at * last_im + through * first_im,
            bt + through * first_by,
        )
    next_re, next_im = zero, zero
    firsts[groups, 0] = zero
    firsts[groups, 1] = zero
    for g in reversed(range(groups)):
        first_re, first_im, first_by, last_re, last_im, last_by = eliminated[g]
        next_re = first_re + first_by * next_re
        next_im = first_im + first_by * next_im
        firsts[g, 0] = next_re
        firsts[g, 1] = next_im
        lasts[g, 0] = last_re + last_by * next_re
        lasts[g, 1] = last_im + last_by * next_im
    left_re, left_im = lasts[own, 0], lasts[own, 1]
    right_re, right_im = firsts[own + 1, 0], firsts[own + 1, 1]

    def join(i, carry):
        at = rows8(i)
        a, b = aa[at, :], bb[at, :]
        pre[at, :] = yre[at, :] + a * left_re + b * right_re
        pim[at, :] = yim[at, :] + a * left_im + b * right_im
        return carry

    lax.fori_loop(0, depth, join, 0, unroll=8)
    for k1 in range(radix):
        for z in range(0, depth, 16):
            at = slice(z, z + 16)
            for half, full in ((slice(None, inner), pre), (slice(inner, None), pim)):
                both = jnp.concatenate(
                    [
                        full[pl.ds(8 * z + k1, 8, stride=8), :],
                        full[pl.ds(8 * z + 64 + k1, 8, stride=8), :],
                    ]
                )
                high, low = split(both)
                phi[k1, at, half] = high
                plo[k1, at, half] = low
        dot = functools.partial(
            lax.dot_general, dimension_numbers=NT, preferred_element_type=f32
        )
        mixed[k1] = (
            dot(thi[k1], phi[k1]) + dot(thi[k1], plo[k1]) + dot(tlo[k1], phi[k1])
        )

    def unmix(i, carry):
        at = pl.ds(pl.multiple_of(i * 16, 16), 16)
        lower = pl.ds(pl.multiple_of(i * 16 + inner, 16), 16)
        for z in range(0, depth, 128):
            lanes = slice(z, z + 128)
            re = [mixed[k1, at, lanes] for k1 in range(radix)]
            im = [mixed[k1, lower, lanes] for k1 in range(radix)]
            re, im = butterfly(re, im, 1)
            for r in range(radix):
                done[r, 0, at, lanes] = re[r].astype(bf16)
                done[r, 1, at, lanes] = im[r].astype(bf16)
        return carry

    lax.fori_loop(0, inner // 16, unmix, 0)
    for s in range(rows):
        start = (me[0] ^ s) * xb
        group = start // inner
        offset = pl.multiple_of(start % inner, xb)
        pieces[s][...] = done[group, :, pl.ds(offset, xb), :]


def spread_kernel(rows, me, *rest):
    pieces, out = rest[:rows], rest[rows]
    for s in range(rows):
        out[:, me[0] ^ s] = pieces[s][...].astype(f32)


def band_coefficients(cell_width):
    length = cell_width.shape[0]
    index = jnp.arange(length, dtype=jnp.int32)
    previous = jnp.concatenate([cell_width[:1], cell_width[:-1]])
    following = jnp.concatenate([cell_width[1:], cell_width[-1:]])
    lower_band = jnp.where(index > 0, 1.0 / (0.5 * (previous + cell_width) * cell_width), 0.0)
    upper_band = jnp.where(
        index < length - 1, 1.0 / (0.5 * (cell_width + following) * cell_width), 0.0
    )
    return (lower_band, upper_band)


def exchange(pieces, axis):
    size = lax.axis_size(axis)
    got = [pieces[0]] + [None] * (size - 1)
    for s in reversed(range(1, size)):
        got[s] = lax.ppermute(pieces[s], axis, [(i, i ^ s) for i in range(size)])
    return got


def on_device(velocity_x, velocity_y, velocity_z, spacing, level_index, plane_index):
    parts, planes, xb, depth = velocity_x.shape
    rows = lax.axis_size("row")
    groups = lax.axis_size("gz")
    total_x = xb * rows
    inner = total_x // RADIX
    row_id = lax.axis_index("row")
    group_id = lax.axis_index("gz")
    me = jnp.stack([row_id, group_id]).astype(jnp.int32)
    assert planes == rows and rows & (rows - 1) == 0 and groups & (groups - 1) == 0
    assert inner % xb == 0

    piece = shape_of((parts, xb, depth), bf16)
    packed = pl.pallas_call(
        functools.partial(pack_kernel, rows),
        out_shape=[shape_of((parts * planes, xb), bf16)] + [piece] * rows,
        grid=(1,),
        in_specs=[
            SMEM,
            pl.BlockSpec((parts, planes, xb, depth), lambda i: (0, 0, 0, 0)),
            pl.BlockSpec(
                (parts, planes, xb, 128), lambda i: (0, 0, 0, depth // 128 - 1)
            ),
        ],
        out_specs=[VMEM] * (rows + 1),
        compiler_params=pltpu.CompilerParams(vmem_limit_bytes=24 << 20),
        cost_estimate=pl.CostEstimate(
            flops=10**8, bytes_accessed=1 << 21, transcendentals=0
        ),
    )(me, velocity_x, velocity_z)
    wall = lax.ppermute(packed[0], "gz", [(i, i + 1) for i in range(groups - 1)])
    along = exchange(packed[1:], "row")

    levels = spacing.shape[0]
    onehot = (level_index[:, None] == jnp.arange(levels, dtype=jnp.int32)[None, :]).astype(f32)
    cell_width = jnp.sum(onehot * spacing[None, :], axis=1)
    lower_band, upper_band = band_coefficients(cell_width)
    own_width = lax.dynamic_slice_in_dim(cell_width, group_id * depth, depth)
    own_lower = lax.dynamic_slice_in_dim(lower_band, group_id * depth, depth)
    own_upper = lax.dynamic_slice_in_dim(upper_band, group_id * depth, depth)
    wave_y = plane_index.astype(f32) * wave_unit
    modes = (
        jnp.arange(inner, dtype=jnp.int32)[None, :] * RADIX
        + jnp.arange(RADIX, dtype=jnp.int32)[:, None]
    )
    signed = jnp.where(modes >= total_x // 2, modes - total_x, modes)
    wave_x = signed.astype(f32) * (full_turn / total_x)
    own_wave = lax.dynamic_slice_in_dim(wave_y, row_id, 1)
    wave_sq = wave_x * wave_x + own_wave * own_wave

    sources = call(
        functools.partial(source_kernel, rows),
        [piece] * rows,
        [SMEM, SMEM] + [VMEM] * 4,
        scratch=[pltpu.VMEM((planes, parts, xb, depth), bf16)],
    )(me, wave_y, velocity_y, velocity_z, wall, own_width[None, :])
    spread = exchange(sources, "row")

    line = shape_of((depth * RADIX, inner), f32)
    table = shape_of((RADIX, 2 * inner, 2 * inner), bf16)
    thi, tlo, inv, alp, cut, mid, aa, bb = call(
        functools.partial(prepare_kernel, total_x),
        [table, table, line, line, line, shape_of((RADIX, inner), f32), line, line],
        [SMEM, SMEM, VMEM, ANY],
        flops=4e9,
    )(own_lower, own_upper, wave_sq, sources[0])

    work = [
        pltpu.VMEM((RADIX, parts, inner, depth), bf16),
        pltpu.VMEM((RADIX, depth, 2 * inner), f32),
        pltpu.VMEM((RADIX, depth, 2 * inner), bf16),
        pltpu.VMEM((RADIX, depth, 2 * inner), bf16),
    ]
    lines = pltpu.VMEM((depth * RADIX, inner), f32)
    gre, gim = call(
        functools.partial(along_kernel, rows),
        [line, line],
        [SMEM] + [VMEM] * (3 + rows),
        scratch=work,
        flops=2e9,
    )(me, wave_x, thi, tlo, *along)

    yre, yim, edges = call(
        functools.partial(solve_kernel, rows),
        [line, line, shape_of((8 * RADIX, inner), f32)],
        [SMEM] + [VMEM] * (10 + rows - 0),
        scratch=work + [lines, lines],
        flops=2e9,
    )(me, thi, tlo, inv, alp, cut, mid, aa, bb, gre, gim, *spread)

    every = exchange([edges] * groups, "gz")
    pieces = call(
        functools.partial(back_kernel, rows, groups),
        [piece] * rows,
        [SMEM] + [VMEM] * (6 + groups),
        scratch=[
            pltpu.VMEM((groups, 8 * RADIX, inner), f32),
            pltpu.VMEM((groups + 1, 2, RADIX, inner), f32),
            pltpu.VMEM((groups, 2, RADIX, inner), f32),
            lines,
            lines,
            pltpu.VMEM((RADIX, depth, 2 * inner), bf16),
            pltpu.VMEM((RADIX, depth, 2 * inner), bf16),
            pltpu.VMEM((RADIX, 2 * inner, depth), f32),
            pltpu.VMEM((RADIX, parts, inner, depth), bf16),
        ],
        flops=2e9,
    )(me, thi, tlo, aa, bb, yre, yim, *every)

    back = exchange(pieces, "row")
    return call(
        functools.partial(spread_kernel, rows),
        shape_of((parts, planes, xb, depth), f32),
        [SMEM] + [VMEM] * rows,
    )(me, *back)


def solution(mesh):
    placed = (
        P(None, None, "row", "gz"),
        P(None, None, "row", "gz"),
        P(None, None, "row", "gz"),
        P(),
        P(),
        P(),
    )
    return jax.shard_map(
        on_device, mesh=mesh, in_specs=placed, out_specs=P(None, None, "row", "gz"), check_vma=False
    )
```
